32 devices in a mesh: branch: 4 (over x, core), shard: 8 (over z, y).
Axes of the slice: x: 2, y: 2, z: 4, core: 2. Of those that a mesh axis runs over, the one named last changes fastest.
Arguments:
- attention_weights: bfloat16 [4, 2, 4096, 4096], P('branch', None, None, 'shard'), may hold values from -1.25 to 1.25
- ffn_weights: bfloat16 [4, 3, 4096, 11008], P('branch', None, 'shard'), may hold values from -0.3125 to 0.3125
- tokens: bfloat16 [512, 4096], P(('branch', 'shard')), may hold values from -6 to 6
- routes: int32 [512, 2], P(('branch', 'shard')), may hold values from 0 to 3, all different within a row; in each aligned block of 16 rows (0 to 15, 16 to 31, ...) at most 12 rows name the same one
- router: bfloat16 [4096, 4], replicated, may hold values from -0.09375 to 0.09375
Outputs:
- merged_attention: bfloat16 [2, 4096, 4096], P(None, 'branch', 'shard')
- expert_weights: bfloat16 [4, 3, 4096, 11008], P('branch', None, None, 'shard')
- mixed_output: bfloat16 [512, 4096], P(('branch', 'shard'))
The draws below stay inside these ranges and needn't reach their ends.
Inputs may be any that keep to these rules, and one draw needn't show every extreme that they name: `routes`: the 2 experts of a row differ. In each aligned block of 16 rows (the rows of one device) no expert is named by more than 12 rows, and in some blocks one expert is named by exactly 12 rows.
All inputs are finite; a program needn't handle non-finite values.
Results may differ from the reference program's by a relative error of at most 0.018.
Values may be sent and summed in bfloat16 or wider, within the bound.
A program may use at most 256 MiB of HBM per device.

```python
import math
import jax
import jax.numpy as jnp
import numpy as np
from jax import lax

D = 4096
FF = 11008
ATT_MATS = 2
TOP = 2
TOK_DEV = 16
CAP = 12
EXPERTS = 4
TOKENS = 512
N_BRANCH = 4
N_SHARD = 8
DEVICES = 32


def block_scale(key, dims, pieces, low, top_value):
    level, own = 1.0, jax.random.fold_in(key, 6)
    for dim, shards_of in pieces:
        steps = jnp.exp(jax.random.uniform(jax.random.fold_in(own, dim), (shards_of,), jnp.float32, low / len(pieces), top_value / len(pieces)))
        level = level * jnp.repeat(steps, dims[dim] // shards_of).reshape([-1 if axis == dim else 1 for axis in range(len(dims))])
    return level


def routed_block(own_key, own, number, rows, count, top, most, lean):
    order = jax.random.permutation(own_key, count)
    crowded, common = portions_of(count, rows * top, most, lean, True), portions_of(count, rows * top, most, lean, False)
    places = jnp.arange(count)

    def named(sizes, offset_by):
        used = int((sizes > 0).sum())
        fixed = max(1, used // 4)
        passed = fixed + (places - fixed + offset_by * (used - fixed)) % max(1, count - fixed)
        return jnp.zeros((count,), jnp.int32).at[order[jnp.where(places < fixed, places, passed)]].set(jnp.asarray(sizes, jnp.int32))

    sizes = jnp.where(number % 4 == 0, named(crowded, number // 4), named(common, number - number // 4 - 1))
    mixed = jax.random.permutation(jax.random.fold_in(own, 3), count)
    source_of, sink = mixed[0:count // 2 * 2:2], mixed[1:count // 2 * 2:2]
    room = jnp.minimum(sizes[source_of] - 1, most - sizes[sink]) // 2
    room = jnp.where((source_of == order[0]) | (sink == order[0]) | (sizes[sink] == 0), 0, jnp.maximum(room, 0))
    passed = jax.random.randint(jax.random.fold_in(own, 4), (count // 2,), 0, 1 << 20) % (room + 1)
    sizes = sizes.at[source_of].add(-passed).at[sink].add(passed)
    labels = jnp.searchsorted(jnp.cumsum(sizes), jnp.arange(rows * top), side="right").astype(jnp.int32)
    table = labels.reshape(top, rows).T
    table = table[jax.random.permutation(jax.random.fold_in(own, 1), rows)]
    offset_by = jax.random.randint(jax.random.fold_in(own, 2), (rows, 1), 0, top)
    return jnp.take_along_axis(table, (jnp.arange(top)[None, :] + offset_by) % top, axis=1)


def portions_of(amount, total, most, slope, full):
    portions = [(1 << 20) // math.isqrt(rank ** slope) + 1 for rank in range(1, amount + 1)]
    largest = most if full else min(most, max(-(-total // amount), total * portions[0] // sum(portions)))
    least = 1 if total - largest >= amount - 1 else 0
    given, surplus = [largest] + [least] * (amount - 1), total - largest - least * (amount - 1)
    while surplus > 0:
        free = [i for i in range(1, amount) if given[i] < largest] or [i for i in range(1, amount) if given[i] < most]
        whole, budget = sum([portions[i] for i in free]), surplus
        for i in free:
            more = min(most - given[i], max(1, budget * portions[i] // whole), surplus)
            given[i] = given[i] + more
            surplus = surplus - more
    return np.array(given)


def scatter_about(key, shape, scale, most, split=(), kind=jnp.bfloat16):
    array = jax.random.normal(key, shape, jnp.float32) * scale
    if len(split) > 0:
        array = block_scale(key, shape, split, -0.22, 0.18) * array
    return jnp.clip(array, min=-most, max=most).astype(kind)


def setup_inputs(seed: int = 0) -> dict:
    splits = jax.random.split(jax.random.key(seed), 6)
    attention_weights = scatter_about(splits[0], (EXPERTS, ATT_MATS, D, D), 0.08, 1.25, ((0, 4), (3, 8)))
    ffn_weights = scatter_about(splits[1], (EXPERTS, 3, D, FF), 0.02, 0.3125, ((0, 4), (2, 8)))
    tokens = scatter_about(splits[2], (TOKENS, D), 1.0, 6.0, ((0, 32),))
    routes_keys = jax.random.split(jax.random.fold_in(splits[3], 1), TOKENS // TOK_DEV)
    routes_turns = jax.random.permutation(jax.random.fold_in(splits[3], 3), TOKENS // TOK_DEV)
    routes = jax.vmap(lambda own, number: routed_block(jax.random.fold_in(splits[3], 2), own, number, TOK_DEV, EXPERTS, TOP, CAP, 1))(routes_keys, routes_turns).reshape((TOKENS, TOP))
    router = scatter_about(splits[4], (D, EXPERTS), D ** -0.5, 0.09375)
    return {"attention_weights": attention_weights, "ffn_weights": ffn_weights, "tokens": tokens, "routes": routes, "router": router}


def slot_table(route_rows, experts_count, capacity):
    chosen = (route_rows[:, :, None] == jnp.arange(experts_count, dtype=jnp.int32)).astype(jnp.int32)
    flat_picks = chosen.reshape(-1, experts_count)
    before = jnp.cumsum(flat_picks, axis=0) - flat_picks
    position = jnp.sum(before * flat_picks, axis=1)
    slot_id = route_rows.reshape(-1) * capacity + position
    one_hot = (slot_id[:, None] == jnp.arange(experts_count * capacity, dtype=jnp.int32)).astype(jnp.float32)
    return jnp.sum(one_hot.reshape(route_rows.shape[0], route_rows.shape[1], -1), axis=1)


def expert_output(slot_rows, weights):
    gate_proj = jnp.dot(slot_rows, weights[0], preferred_element_type=jnp.float32)
    up_proj = jnp.dot(slot_rows, weights[1], preferred_element_type=jnp.float32)
    hidden = (jax.nn.silu(gate_proj) * up_proj).astype(jnp.bfloat16)
    part_width = FF // N_SHARD

    def add_part(summed, column):
        offset = column * part_width
        hidden_part = lax.dynamic_slice_in_dim(hidden, offset, part_width, 1)
        down_part = lax.dynamic_slice_in_dim(weights[2], offset, part_width, 1)
        partial_value = lax.dot_general(hidden_part, down_part, (((1,), (1,)), ((), ())), preferred_element_type=jnp.float32)
        rounded = lax.optimization_barrier(partial_value.astype(jnp.bfloat16))
        return summed + rounded.astype(jnp.float32), None

    initial = jnp.zeros((slot_rows.shape[0], weights.shape[1]), jnp.float32)
    summed, unused = lax.scan(add_part, initial, jnp.arange(N_SHARD, dtype=jnp.int32))
    return summed.astype(jnp.bfloat16)


def reference(attention_weights, ffn_weights, tokens, routes, router):
    attention_sum = jnp.sum(attention_weights.astype(jnp.float32), axis=0)
    merged_attention = (attention_sum * (1.0 / N_BRANCH)).astype(jnp.bfloat16)
    device_tokens = tokens.reshape(DEVICES, TOK_DEV, D)
    device_routes = routes.reshape(DEVICES, TOK_DEV, TOP)
    tables = jax.vmap(lambda route_rows: slot_table(route_rows, EXPERTS, CAP))(device_routes)
    buffers = jnp.einsum("dts,dtf->dsf", tables, device_tokens.astype(jnp.float32)).astype(jnp.bfloat16)
    per_expert = buffers.reshape(DEVICES, EXPERTS, CAP, D).transpose(1, 0, 2, 3).reshape(EXPERTS, DEVICES * CAP, D)
    results = lax.map(lambda expert_pair: expert_output(expert_pair[0], expert_pair[1]), (per_expert, ffn_weights))
    returned = results.reshape(EXPERTS, DEVICES, CAP, D).transpose(1, 0, 2, 3).reshape(DEVICES, EXPERTS * CAP, D)
    gates_all = jax.nn.sigmoid(jnp.dot(tokens, router, preferred_element_type=jnp.float32)).reshape(DEVICES, TOK_DEV, EXPERTS)
    weighting = tables * jnp.repeat(gates_all, CAP, axis=2)
    mixed_output = jnp.einsum("dts,dsf->dtf", weighting, returned.astype(jnp.float32), precision=lax.Precision.HIGHEST)
    mixed_output = mixed_output.astype(jnp.bfloat16).reshape(TOKENS, D)
    return merged_attention, ffn_weights, mixed_output
```

```python
import functools

import jax
import jax.numpy as jnp
from jax import lax
from jax.experimental import pallas as pl
from jax.experimental.pallas import tpu as pltpu
from jax.sharding import PartitionSpec as P

LANES = 128


def far_first(outer, inner):
    order = sorted(range(outer), key=lambda step: abs(2 * step - outer))
    return [(o, i) for o in order for i in range(inner - 1, -1, -1) if o or i]


def moved(place, step, outer, inner):
    return lax.rem(place // inner + step[0] + outer, outer) * inner + lax.rem(
        place % inner + step[1] + inner, inner
    )


def pack_kernel(info_ref, x_ref, after_ref, o_ref, turned_ref):
    turned_ref[...] = x_ref[0, 0].astype(turned_ref.dtype).T
    width = o_ref.shape[1]
    unit = 16 if turned_ref.dtype == jnp.bfloat16 else 8
    first = pl.multiple_of(info_ref[1], unit)
    o_ref[0] = turned_ref[pl.ds(first, width), :].astype(o_ref.dtype)


def pack(ffn, mats, rows, target, width, after):
    first, count = mats
    low, height = rows
    ff = ffn.shape[3]
    window = min(-(-(width + LANES - 1) // LANES) * LANES, ff)
    start = jnp.minimum(target * width // LANES, (ff - window) // LANES)
    tile = max(t for t in (2 * LANES, LANES) if height % t == 0)
    kind = jnp.bfloat16 if width % 16 == 0 else jnp.float32
    return pl.pallas_call(
        pack_kernel,
        grid_spec=pltpu.PrefetchScalarGridSpec(
            num_scalar_prefetch=1,
            grid=(count, height // tile),
            in_specs=[
                pl.BlockSpec(
                    (pl.Element(1), pl.Element(1), pl.Element(tile), pl.Element(window)),
                    lambda m, r, t: (
                        0,
                        m + first,
                        pl.multiple_of(low + r * tile, LANES),
                        pl.multiple_of(t[0] * LANES, LANES),
                    ),
                ),
                pl.BlockSpec(memory_space=pl.ANY),
            ],
            out_specs=pl.BlockSpec((1, width, tile), lambda m, r, t: (m, 0, r)),
            scratch_shapes=[pltpu.VMEM((window, tile), kind)],
        ),
        out_shape=jax.ShapeDtypeStruct((count, width, height), ffn.dtype),
        cost_estimate=pl.CostEstimate(
            flops=0, bytes_accessed=5 * count * height * width, transcendentals=0
        ),
    )(jnp.stack([start, target * width - start * LANES]).astype(jnp.int32), ffn, after)


def gate_up_kernel(info_ref, rows_ref, piece_ref, *refs):
    total_ref, out_ref = refs[-2:]
    total = lax.dot_general(
        rows_ref[...], piece_ref[0], (((1,), (1,)), ((), ())), preferred_element_type=jnp.float32
    )
    total_ref[0] = refs[0][0] + total if len(refs) > 2 else total
    out_ref[0] = piece_ref[0]


def gate_up_step(all_rows, source, piece, carried, shape):
    count, width, depth = piece.shape
    rows = all_rows.shape[0]
    total_spec = pl.BlockSpec((1, rows, width), lambda m, t: (m, 0, 0))
    return pl.pallas_call(
        gate_up_kernel,
        grid_spec=pltpu.PrefetchScalarGridSpec(
            num_scalar_prefetch=1,
            grid=(count,),
            in_specs=[
                pl.BlockSpec((rows, depth), lambda m, t: (0, t[0])),
                pl.BlockSpec((1, width, depth), lambda m, t: (m, 0, 0)),
            ]
            + [total_spec, pl.BlockSpec(memory_space=pl.ANY)][: len(carried)],
            out_specs=[total_spec, pl.BlockSpec((1, width, depth), lambda m, t: (m, 0, t[0]))],
        ),
        out_shape=[
            jax.ShapeDtypeStruct((count, rows, width), jnp.float32),
            jax.ShapeDtypeStruct(shape, piece.dtype),
        ],
        input_output_aliases={3 + i: i for i in range(len(carried))},
        cost_estimate=pl.CostEstimate(
            flops=2 * count * rows * depth * width,
            bytes_accessed=count * width * (4 * depth + 8 * rows),
            transcendentals=0,
        ),
    )(jnp.stack([source]).astype(jnp.int32), all_rows, piece, *carried)


def down_kernel(steps, sizes, low, hidden_ref, weight_ref, *refs):
    pieces, (partial_ref, out_ref, sems) = refs[: len(steps)], refs[-3:]
    me = lax.axis_index("shard")
    last = out_ref.shape[0] - 1
    height = pieces[0].shape[2]
    depth = out_ref.shape[2] // partial_ref.shape[0]
    copies = []
    for k, (step, piece_ref) in enumerate(zip(steps, pieces)):
        columns = pl.ds(pl.multiple_of(moved(me, step, *sizes) * depth + low, LANES), height)
        copy = pltpu.make_async_copy(piece_ref.at[0], out_ref.at[last, :, columns], sems.at[k])
        copy.start()
        copies.append(copy)
    for step, piece_ref in zip(steps, pieces):
        columns = jnp.dot(hidden_ref[...], piece_ref[0], preferred_element_type=jnp.float32)
        partial_ref[moved(me, step, *sizes)] = (columns * weight_ref[...]).astype(partial_ref.dtype)
    for copy in copies:
        copy.wait()


def down(hidden, weight, steps, sizes, pieces, low, weights):
    _, width, height = pieces[0].shape
    rows, shards = hidden.shape[0], len(pieces)
    return pl.pallas_call(
        functools.partial(down_kernel, steps, sizes, low),
        grid=(1,),
        in_specs=[
            pl.BlockSpec((rows, width), lambda i: (0, 0)),
            pl.BlockSpec((rows, 1), lambda i: (0, 0)),
        ]
        + [pl.BlockSpec((1, width, height), lambda i: (0, 0, 0))] * shards
        + [pl.BlockSpec(memory_space=pl.ANY)],
        out_specs=[
            pl.BlockSpec((shards, rows, height), lambda i: (0, 0, 0)),
            pl.BlockSpec(memory_space=pl.ANY),
        ],
        out_shape=[
            jax.ShapeDtypeStruct((shards, rows, height), jnp.bfloat16),
            jax.ShapeDtypeStruct(weights.shape, weights.dtype),
        ],
        scratch_shapes=[pltpu.SemaphoreType.DMA((shards,))],
        input_output_aliases={2 + shards: 1},
        cost_estimate=pl.CostEstimate(
            flops=2 * rows * height * width * shards,
            bytes_accessed=shards * height * (4 * width + 2 * rows) + 2 * rows * width,
            transcendentals=0,
        ),
    )(hidden, weight, *pieces, weights)


def from_ahead(x, step, outer, inner):
    pairs = [
        (((o + step[0]) % outer) * inner + (i + step[1]) % inner, o * inner + i)
        for o in range(outer)
        for i in range(inner)
    ]
    return lax.ppermute(x, "shard", pairs)


def from_branch(x, step):
    count = lax.axis_size("branch")
    return lax.ppermute(x, "branch", [((b + step) % count, b) for b in range(count)])


def gather_all(x, outer, inner):
    x = jnp.concatenate([x] + [from_ahead(x, (k, 0), outer, inner) for k in range(1, outer)])
    x = jnp.concatenate([x] + [from_ahead(x, (0, k), outer, inner) for k in range(1, inner)])
    others = range(1, lax.axis_size("branch"))
    return jnp.concatenate([x] + [from_branch(x, k) for k in others])


def add_up(pieces):
    return functools.reduce(lambda a, b: a + b, [p.astype(jnp.float32) for p in pieces])


def scatter_sum(x, outer, inner):
    def stage(x, count, move):
        parts = jnp.split(x, count, axis=1)
        return add_up([parts[0]] + [move(parts[k], count - k) for k in range(1, count)])

    x = stage(x, lax.axis_size("branch"), from_branch).astype(jnp.bfloat16)
    move = lambda p, k: from_ahead(p, (0, k), outer, inner)
    x = stage(x, inner, move).astype(jnp.bfloat16)
    move = lambda p, k: from_ahead(p, (k, 0), outer, inner)
    return stage(x, outer, move).astype(jnp.bfloat16)


def local(attention_weights, ffn_weights, tokens, routes, router):
    branches = lax.axis_size("branch")
    shards = lax.axis_size("shard")
    inner = 2 if shards % 2 == 0 else 1
    outer = shards // inner
    me = lax.axis_index("shard")
    expert = lax.axis_index("branch")
    every, depth = ffn_weights.shape[1:3]
    width = ffn_weights.shape[3] // shards
    model_width = shards * depth
    own_rows = tokens.shape[0]

    chosen = jnp.any(routes[:, :, None] == jnp.arange(branches, dtype=jnp.int32), axis=1)
    chosen = jnp.pad(chosen.astype(tokens.dtype), ((0, 0), (0, LANES - branches)))
    all_rows = gather_all(jnp.concatenate([tokens, chosen], axis=1), outer, inner)

    low = max(depth - LANES, 0)
    groups = [((0, 2), (0, depth))]
    groups += [((2, 1), rows) for rows in ((0, low), (low, depth - low)) if rows[1]]
    order = far_first(outer, inner)
    backs = [(0, 0)] + [(outer - o, inner - i) for o, i in order]
    after = routes
    own, arrivals, number = [], [], 0
    for mats, rows in groups:
        pieces = []
        for step in order:
            after = pack(ffn_weights, mats, rows, moved(me, step, outer, inner), width, after)
            pieces.append(from_ahead(after, (outer - step[0], inner - step[1]), outer, inner))
            number += 1
        arrivals.append(pieces)
    for mats, rows in groups:
        own.append(pack(ffn_weights, mats, rows, me, width, after))

    gates = jax.nn.sigmoid(
        jnp.dot(all_rows[:, :model_width], router, preferred_element_type=jnp.float32)
    )
    picked = all_rows[:, model_width : model_width + branches].astype(jnp.float32)
    mine = (jnp.arange(branches) == expert).astype(jnp.float32)
    weight = jnp.sum(gates * picked * mine, axis=1, keepdims=True)

    carried = ()
    shape = (every, width, model_width)
    for at, piece in enumerate([own[0]] + arrivals[0]):
        source = moved(me, backs[at], outer, inner)
        carried = gate_up_step(all_rows, source, piece, carried, shape)
    total, weights = carried
    hidden = (jax.nn.silu(total[0]) * total[1]).astype(jnp.bfloat16)

    mixed = []
    for group in range(1, len(groups)):
        pieces = [own[group]] + arrivals[group]
        partial, weights = down(
            hidden, weight, backs, (outer, inner), pieces, groups[group][1][0], weights
        )
        mixed.append(scatter_sum(partial, outer, inner))
    mixed_output = jnp.concatenate(mixed, axis=2).transpose(1, 0, 2).reshape(own_rows, model_width)
    expert_weights = weights.transpose(0, 2, 1)[None]

    share = attention_weights.shape[2] // branches
    pieces = []
    for step in range(branches):
        rows = lax.rem(expert + step, branches) * share
        block = lax.dynamic_slice_in_dim(attention_weights[0], rows, share, 1)
        pieces.append(from_branch(block, branches - step) if step else block)
    merged_attention = (add_up(pieces) * (1.0 / branches)).astype(jnp.bfloat16)
    return (merged_attention, expert_weights, mixed_output)


def solution(mesh):
    placed = (
        P("branch", None, None, "shard"),
        P("branch", None, "shard", None),
        P(("branch", "shard"), None),
        P(("branch", "shard"), None),
        P(),
    )
    return jax.shard_map(
        local,
        mesh=mesh,
        in_specs=placed,
        out_specs=(
            P(None, "branch", "shard"),
            P("branch", None, None, "shard"),
            P(("branch", "shard"), None),
        ),
        check_vma=False,
    )
```

```python
import functools

import jax
import jax.numpy as jnp
from jax import lax
from jax.experimental import pallas as pl
from jax.experimental.pallas import tpu as pltpu
from jax.sharding import PartitionSpec as P

LANES = 128


def far_first(outer, inner):
    order = sorted(range(outer), key=lambda step: abs(2 * step - outer))
    return [(o, i) for o in order for i in range(inner - 1, -1, -1) if o or i]


def moved(place, step, outer, inner):
    return lax.rem(place // inner + step[0] + outer, outer) * inner + lax.rem(
        place % inner + step[1] + inner, inner
    )


def pack_kernel(info_ref, x_ref, after_ref, o_ref, turned_ref):
    turned_ref[...] = x_ref[0, 0].astype(turned_ref.dtype).T
    width = o_ref.shape[1]
    unit = 16 if turned_ref.dtype == jnp.bfloat16 else 8
    first = pl.multiple_of(info_ref[1], unit)
    o_ref[0] = turned_ref[pl.ds(first, width), :].astype(o_ref.dtype)


def pack(ffn, mats, rows, target, width, after):
    first, count = mats
    low, height = rows
    ff = ffn.shape[3]
    window = min(-(-(width + LANES - 1) // LANES) * LANES, ff)
    start = jnp.minimum(target * width // LANES, (ff - window) // LANES)
    tile = max(t for t in (2 * LANES, LANES) if height % t == 0)
    kind = jnp.bfloat16 if width % 16 == 0 else jnp.float32
    return pl.pallas_call(
        pack_kernel,
        grid_spec=pltpu.PrefetchScalarGridSpec(
            num_scalar_prefetch=1,
            grid=(count, height // tile),
            in_specs=[
                pl.BlockSpec(
                    (pl.Element(1), pl.Element(1), pl.Element(tile), pl.Element(window)),
                    lambda m, r, t: (
                        0,
                        m + first,
                        pl.multiple_of(low + r * tile, LANES),
                        pl.multiple_of(t[0] * LANES, LANES),
                    ),
                ),
                pl.BlockSpec(memory_space=pl.ANY),
            ],
            out_specs=pl.BlockSpec((1, width, tile), lambda m, r, t: (m, 0, r)),
            scratch_shapes=[pltpu.VMEM((window, tile), kind)],
        ),
        out_shape=jax.ShapeDtypeStruct((count, width, height), ffn.dtype),
        cost_estimate=pl.CostEstimate(
            flops=0, bytes_accessed=5 * count * height * width, transcendentals=0
        ),
    )(jnp.stack([start, target * width - start * LANES]).astype(jnp.int32), ffn, after)


def gate_up_kernel(info_ref, rows_ref, piece_ref, *refs):
    total_ref, out_ref = refs[-2:]
    total = lax.dot_general(
        rows_ref[...], piece_ref[0], (((1,), (1,)), ((), ())), preferred_element_type=jnp.float32
    )
    total_ref[0] = refs[0][0] + total if len(refs) > 2 else total
    out_ref[0] = piece_ref[0]


def gate_up_step(all_rows, source, piece, carried, shape):
    count, width, depth = piece.shape
    rows = all_rows.shape[0]
    total_spec = pl.BlockSpec((1, rows, width), lambda m, t: (m, 0, 0))
    return pl.pallas_call(
        gate_up_kernel,
        grid_spec=pltpu.PrefetchScalarGridSpec(
            num_scalar_prefetch=1,
            grid=(count,),
            in_specs=[
                pl.BlockSpec((rows, depth), lambda m, t: (0, t[0])),
                pl.BlockSpec((1, width, depth), lambda m, t: (m, 0, 0)),
            ]
            + [total_spec, pl.BlockSpec(memory_space=pl.ANY)][: len(carried)],
            out_specs=[total_spec, pl.BlockSpec((1, width, depth), lambda m, t: (m, 0, t[0]))],
        ),
        out_shape=[
            jax.ShapeDtypeStruct((count, rows, width), jnp.float32),
            jax.ShapeDtypeStruct(shape, piece.dtype),
        ],
        input_output_aliases={3 + i: i for i in range(len(carried))},
        cost_estimate=pl.CostEstimate(
            flops=2 * count * rows * depth * width,
            bytes_accessed=count * width * (4 * depth + 8 * rows),
            transcendentals=0,
        ),
    )(jnp.stack([source]).astype(jnp.int32), all_rows, piece, *carried)


def down_kernel(steps, sizes, low, hidden_ref, weight_ref, *refs):
    pieces, (partial_ref, out_ref, sems) = refs[: len(steps)], refs[-3:]
    me = lax.axis_index("shard")
    last = out_ref.shape[0] - 1
    height = pieces[0].shape[2]
    depth = out_ref.shape[2] // partial_ref.shape[0]
    copies = []
    for k, (step, piece_ref) in enumerate(zip(steps, pieces)):
        columns = pl.ds(pl.multiple_of(moved(me, step, *sizes) * depth + low, LANES), height)
        copy = pltpu.make_async_copy(piece_ref.at[0], out_ref.at[last, :, columns], sems.at[k])
        copy.start()
        copies.append(copy)
    for step, piece_ref in zip(steps, pieces):
        columns = jnp.dot(hidden_ref[...], piece_ref[0], preferred_element_type=jnp.float32)
        partial_ref[moved(me, step, *sizes)] = (columns * weight_ref[...]).astype(partial_ref.dtype)
    for copy in copies:
        copy.wait()


def down(hidden, weight, steps, sizes, pieces, low, weights):
    _, width, height = pieces[0].shape
    rows, shards = hidden.shape[0], len(pieces)
    return pl.pallas_call(
        functools.partial(down_kernel, steps, sizes, low),
        grid=(1,),
        in_specs=[
            pl.BlockSpec((rows, width), lambda i: (0, 0)),
            pl.BlockSpec((rows, 1), lambda i: (0, 0)),
        ]
        + [pl.BlockSpec((1, width, height), lambda i: (0, 0, 0))] * shards
        + [pl.BlockSpec(memory_space=pl.ANY)],
        out_specs=[
            pl.BlockSpec((shards, rows, height), lambda i: (0, 0, 0)),
            pl.BlockSpec(memory_space=pl.ANY),
        ],
        out_shape=[
            jax.ShapeDtypeStruct((shards, rows, height), jnp.bfloat16),
            jax.ShapeDtypeStruct(weights.shape, weights.dtype),
        ],
        scratch_shapes=[pltpu.SemaphoreType.DMA((shards,))],
        input_output_aliases={2 + shards: 1},
        cost_estimate=pl.CostEstimate(
            flops=2 * rows * height * width * shards,
            bytes_accessed=shards * height * (4 * width + 2 * rows) + 2 * rows * width,
            transcendentals=0,
        ),
    )(hidden, weight, *pieces, weights)


def from_ahead(x, step, outer, inner, axis="shard"):
    pairs = [
        (((o + step[0]) % outer) * inner + (i + step[1]) % inner, o * inner + i)
        for o in range(outer)
        for i in range(inner)
    ]
    return lax.ppermute(x, axis, pairs)


def from_branch(x, step):
    count = lax.axis_size("branch")
    return lax.ppermute(x, "branch", [((b + step) % count, b) for b in range(count)])


def branch_sizes():
    count = lax.axis_size("branch")
    cores = 2 if count % 2 == 0 else 1
    return count // cores, cores


def gather_all(x, outer, inner):
    x = jnp.concatenate([x] + [from_ahead(x, (k, 0), outer, inner) for k in range(1, outer)])
    x = jnp.concatenate([x] + [from_ahead(x, (0, k), outer, inner) for k in range(1, inner)])
    chips, cores = branch_sizes()
    moves = [((k, 0), chips, cores, "branch") for k in range(1, chips)]
    x = jnp.concatenate([x] + [from_ahead(x, *move) for move in moves])
    moves = [((0, k), chips, cores, "branch") for k in range(1, cores)]
    return jnp.concatenate([x] + [from_ahead(x, *move) for move in moves])


def add_up(pieces):
    return functools.reduce(lambda a, b: a + b, [p.astype(jnp.float32) for p in pieces])


def scatter_sum(x, outer, inner):
    def stage(x, count, move):
        parts = jnp.split(x, count, axis=1)
        return add_up([parts[0]] + [move(parts[k], count - k) for k in range(1, count)])

    chips, cores = branch_sizes()
    move = lambda p, k: from_ahead(p, (0, k), chips, cores, "branch")
    x = stage(x, cores, move).astype(jnp.bfloat16)
    move = lambda p, k: from_ahead(p, (k, 0), chips, cores, "branch")
    x = stage(x, chips, move).astype(jnp.bfloat16)
    move = lambda p, k: from_ahead(p, (0, k), outer, inner)
    x = stage(x, inner, move).astype(jnp.bfloat16)
    move = lambda p, k: from_ahead(p, (k, 0), outer, inner)
    return stage(x, outer, move).astype(jnp.bfloat16)


def local(attention_weights, ffn_weights, tokens, routes, router):
    branches = lax.axis_size("branch")
    shards = lax.axis_size("shard")
    inner = 2 if shards % 2 == 0 else 1
    outer = shards // inner
    me = lax.axis_index("shard")
    expert = lax.axis_index("branch")
    every, depth = ffn_weights.shape[1:3]
    width = ffn_weights.shape[3] // shards
    model_width = shards * depth
    own_rows = tokens.shape[0]

    chosen = jnp.any(routes[:, :, None] == jnp.arange(branches, dtype=jnp.int32), axis=1)
    chosen = jnp.pad(chosen.astype(tokens.dtype), ((0, 0), (0, LANES - branches)))
    all_rows = gather_all(jnp.concatenate([tokens, chosen], axis=1), outer, inner)

    low = max(depth - LANES, 0)
    groups = [((0, 2), (0, depth))]
    groups += [((2, 1), rows) for rows in ((0, low), (low, depth - low)) if rows[1]]
    order = far_first(outer, inner)
    backs = [(0, 0)] + [(outer - o, inner - i) for o, i in order]
    after = routes
    own, arrivals, number = [], [], 0
    for mats, rows in groups:
        pieces = []
        for step in order:
            after = pack(ffn_weights, mats, rows, moved(me, step, outer, inner), width, after)
            pieces.append(from_ahead(after, (outer - step[0], inner - step[1]), outer, inner))
            number += 1
        arrivals.append(pieces)
    for mats, rows in groups:
        own.append(pack(ffn_weights, mats, rows, me, width, after))

    gates = jax.nn.sigmoid(
        jnp.dot(all_rows[:, :model_width], router, preferred_element_type=jnp.float32)
    )
    picked = all_rows[:, model_width : model_width + branches].astype(jnp.float32)
    mine = (jnp.arange(branches) == expert).astype(jnp.float32)
    weight = jnp.sum(gates * picked * mine, axis=1, keepdims=True)

    carried = ()
    shape = (every, width, model_width)
    for at, piece in enumerate([own[0]] + arrivals[0]):
        source = moved(me, backs[at], outer, inner)
        carried = gate_up_step(all_rows, source, piece, carried, shape)
    total, weights = carried
    hidden = (jax.nn.silu(total[0]) * total[1]).astype(jnp.bfloat16)

    mixed = []
    for group in range(1, len(groups)):
        pieces = [own[group]] + arrivals[group]
        partial, weights = down(
            hidden, weight, backs, (outer, inner), pieces, groups[group][1][0], weights
        )
        mixed.append(scatter_sum(partial, outer, inner))
    mixed_output = jnp.concatenate(mixed, axis=2).transpose(1, 0, 2).reshape(own_rows, model_width)
    expert_weights = weights.transpose(0, 2, 1)[None]

    share = attention_weights.shape[2] // branches
    pieces = []
    for step in range(branches):
        rows = lax.rem(expert + step, branches) * share
        block = lax.dynamic_slice_in_dim(attention_weights[0], rows, share, 1)
        pieces.append(from_branch(block, branches - step) if step else block)
    merged_attention = (add_up(pieces) * (1.0 / branches)).astype(jnp.bfloat16)
    return (merged_attention, expert_weights, mixed_output)


def solution(mesh):
    placed = (
        P("branch", None, None, "shard"),
        P("branch", None, "shard", None),
        P(("branch", "shard"), None),
        P(("branch", "shard"), None),
        P(),
    )
    return jax.shard_map(
        local,
        mesh=mesh,
        in_specs=placed,
        out_specs=(
            P(None, "branch", "shard"),
            P("branch", None, None, "shard"),
            P(("branch", "shard"), None),
        ),
        check_vma=False,
    )
```
